32 devices in a mesh: row: 8 (over z, x), col: 4 (over y, core).
Axes of the slice: x: 2, y: 2, z: 4, core: 2. Of those that a mesh axis runs over, the one named last changes fastest.
Arguments:
- dense_a: bfloat16 [64, 512, 512], P(('row', 'col')), may hold values from -6 to 6
- dense_b: bfloat16 [64, 512, 512], P(('row', 'col')), may hold values from -0.25 to 0.25
- inner_basis_stack: bfloat16 [64, 2, 512, 128], P(('row', 'col')), may hold values from -0.25 to 0.25
- outer_basis_stack: bfloat16 [64, 2, 512, 128], P(('row', 'col')), may hold values from -1 to 1
- ascent: bfloat16 [32, 4, 2, 128, 128], P(('row', 'col')), may hold values from -0.4375 to 0.4375
- descent: bfloat16 [32, 4, 2, 128, 128], P(('row', 'col')), may hold values from -0.5 to 0.5
- couplings: bfloat16 [32, 2, 4, 128, 128], P(('row', 'col')), may hold values from -0.5 to 0.5
Outputs:
- product_diag: bfloat16 [64, 512, 512], P(('row', 'col'))
The draws below stay inside these ranges and needn't reach their ends.
All inputs are finite; a program needn't handle non-finite values.
Results may differ from the reference program's by a relative error of at most 0.015.
Values may be sent and summed in bfloat16 or wider, within the bound.
A program may use at most 64 MiB of HBM per device.

```python
import jax
import jax.numpy as jnp
from jax import lax

M = 512
R = 128
DEVICES_ALL = 32
LEAVES = 64
N_ROW = 8
N_COL = 4


def block_scale(rng, extent, shards, low, largest):
    level, own = 1.0, jax.random.fold_in(rng, 6)
    for position, shards_of in shards:
        draws = jnp.exp(jax.random.uniform(jax.random.fold_in(own, position), (shards_of,), jnp.float32, low / len(shards), largest / len(shards)))
        level = level * jnp.repeat(draws, extent[position] // shards_of).reshape([-1 if axis == position else 1 for axis in range(len(extent))])
    return level


def scatter_about(own_key, dims, width, reach, shards=(), kind=jnp.bfloat16):
    factor_of = block_scale(own_key, dims, shards, -0.22, 0.18) if shards else 1.0
    drawn = jax.random.normal(own_key, dims, jnp.float32) * width * factor_of
    return jnp.minimum(jnp.maximum(drawn, -reach), reach).astype(kind)


def setup_inputs(seed: int = 0) -> dict:
    keys = jax.random.split(jax.random.key(seed), 8)
    dense_a = scatter_about(keys[0], (LEAVES, M, M), 1.0, 6.0, ((0, 32),))
    dense_b = scatter_about(keys[1], (LEAVES, M, M), M ** -0.5, 0.25, ((0, 32),))
    inner_basis_stack = scatter_about(keys[2], (LEAVES, 2, M, R), M ** -0.5, 0.25, ((0, 32),))
    outer_basis_stack = scatter_about(keys[3], (LEAVES, 2, M, R), (R // 4) ** -0.5, 1.0, ((0, 32),))
    ascent = scatter_about(keys[4], (DEVICES_ALL, 4, 2, R, R), (R * 7 // 5) ** -0.5, 0.4375, ((0, 32),))
    descent = scatter_about(keys[5], (DEVICES_ALL, 4, 2, R, R), R ** -0.5, 0.5, ((0, 32),))
    couplings = scatter_about(keys[6], (DEVICES_ALL, 2, 4, R, R), R ** -0.5, 0.5, ((0, 32),))
    return {"dense_a": dense_a, "dense_b": dense_b, "inner_basis_stack": inner_basis_stack, "outer_basis_stack": outer_basis_stack, "ascent": ascent, "descent": descent, "couplings": couplings}


HIGHEST_PRECISION = lax.Precision.HIGHEST


def multiply(first_arg, second_arg):
    return jnp.matmul(first_arg.astype(jnp.float32), second_arg.astype(jnp.float32), precision=HIGHEST_PRECISION)


def lifted(pair_stack, inner_value):
    return multiply(multiply(jnp.swapaxes(pair_stack[:, 0], 1, 2), inner_value), pair_stack[:, 1])


def lowered(pair_stack, parent):
    return multiply(multiply(pair_stack[:, 0], parent), jnp.swapaxes(pair_stack[:, 1], 1, 2))


def sibling_terms(blocks, inner_value):
    left_terms = multiply(multiply(blocks[:, 0], inner_value[1::2]), blocks[:, 3])
    right_terms = multiply(multiply(blocks[:, 1], inner_value[0::2]), blocks[:, 2])
    return jnp.stack([left_terms, right_terms], 1).reshape(inner_value.shape)


def owners(stacked, height):
    return stacked[2 ** (height - 1) - 1::2 ** height]


def leaf_block(leaf_items):
    first_matrix_block, block_b, bases, mixing = leaf_items
    spread_rows = jnp.dot(bases[0], mixing, preferred_element_type=jnp.float32).astype(jnp.bfloat16)
    result_block = jnp.dot(first_matrix_block, block_b, preferred_element_type=jnp.float32)
    result_block = result_block + jnp.dot(spread_rows, bases[1].T, preferred_element_type=jnp.float32)
    return result_block.astype(jnp.bfloat16)


def reference(dense_a, dense_b, inner_basis_stack, outer_basis_stack, ascent, descent, couplings):
    device_list = N_ROW * N_COL
    levels = device_list.bit_length() - 1
    leaf_inner_product = jnp.einsum('ufw,ufa->uwa', inner_basis_stack[:, 0].astype(jnp.float32),
                            inner_basis_stack[:, 1].astype(jnp.float32), precision=HIGHEST_PRECISION)
    leaf_up = ascent[:, 0:2].reshape(2 * device_list, 2, R, R)
    inner_levels = [leaf_inner_product]
    lifted_terms = lifted(leaf_up, leaf_inner_product)
    current = lifted_terms[0::2] + lifted_terms[1::2]
    inner_levels.append(current)
    for height in range(1, levels + 1):
        if height == 1:
            pair_stack = ascent[:, 2]
        else:
            pair_stack = owners(ascent[:, 3], height - 1)
        lifted_terms = lifted(pair_stack, current)
        current = lifted_terms[0::2] + lifted_terms[1::2]
        inner_levels.append(current)
    coupling = jnp.zeros((1, R, R), jnp.float32)
    for height in range(levels, 0, -1):
        near_terms = sibling_terms(owners(couplings[:, 1], height), inner_levels[height])
        if height == 1:
            pair_stack = descent[:, 2]
        else:
            pair_stack = owners(descent[:, 3], height - 1)
        coupling = near_terms + lowered(pair_stack, jnp.repeat(coupling, 2, axis=0))
    near_terms = sibling_terms(couplings[:, 0], leaf_inner_product)
    leaf_down = descent[:, 0:2].reshape(2 * device_list, 2, R, R)
    leaf_coupling = near_terms + lowered(leaf_down, jnp.repeat(coupling, 2, axis=0))
    rounded_count = leaf_coupling.astype(jnp.bfloat16)
    return lax.map(leaf_block, (dense_a, dense_b, outer_basis_stack, rounded_count))
```

```python
import functools

import jax
import jax.numpy as jnp
from jax import lax
from jax.experimental import pallas as pl
from jax.experimental.pallas import tpu as pltpu
from jax.sharding import PartitionSpec as P

MESH = pl.DeviceIdType.MESH
BF16 = jnp.bfloat16
F32 = jnp.float32
ASC, DESC, COUP = 0, 1, 2


def mm(a, b, ca=1, cb=0):
    return lax.dot_general(
        a.astype(BF16), b.astype(BF16), (((ca,), (cb,)), ((), ())), preferred_element_type=F32
    )


def halves(value):
    high = value.astype(BF16)
    return high, (value - high.astype(F32)).astype(BF16)


def times(value, factor, cb=0):
    if value.dtype == BF16:
        return mm(value, factor, 1, cb)
    rows = value.shape[0]
    both = mm(jnp.concatenate(halves(value), 0), factor, 1, cb)
    return both[:rows] + both[rows:]


def into(factor, value, ca=1):
    if value.dtype == BF16:
        return mm(factor, value, ca, 0)
    columns = value.shape[1]
    both = mm(factor, jnp.concatenate(halves(value), 1), ca, 0)
    return both[:, :columns] + both[:, columns:]


def lift(pair, value):
    return into(pair[0], times(value, pair[1]), 0)


def lower(pair, value):
    return times(into(pair[0], value), pair[1], 1)


def across(first, value, second):
    return times(into(first, value), second)


def tree_kernel(
    levels, columns,
    da_ref, db_ref, inner_ref, outer_ref, asc_ref, desc_ref, coup_ref, o_ref,
    da, db, inner, outer, own_asc, own_desc, own_coup, out, dense,
    table, f_out, t_out, f_in, t_in, near_leaf, near_up,
    load_sem, out_sem, gen_send, gen_recv, up_send, up_recv,
):
    pos = lax.axis_index("row") * columns + lax.axis_index("col")
    bit = [pos // 2**i % 2 for i in range(levels)]
    partner = []
    for i in range(levels):
        other = pos + 2**i * (1 - 2 * bit[i])
        partner.append((other // columns, other % columns))

    low_sum = {}
    for h in range(1, levels + 1):
        total = 0
        for i in range(h):
            total = total + (bit[i] if i == h - 1 else 1 - bit[i])
            low_sum[h, i] = total
    count = {h: low_sum[h, h - 1] for h in range(1, levels + 1)}
    last = {ASC: levels - 2, DESC: levels - 2, COUP: levels}

    barrier = pltpu.get_barrier_semaphore()
    for i in range(levels):
        pl.semaphore_signal(barrier, inc=1, device_id=partner[i], device_id_type=MESH)

    loads = [
        pltpu.make_async_copy(src, dst, load_sem.at[n])
        for n, (src, dst) in enumerate([
            (inner_ref, inner),
            (asc_ref.at[0], own_asc),
            (coup_ref.at[0, 0], own_coup),
            (desc_ref.at[0], own_desc),
            (outer_ref, outer),
            (da_ref, da),
            (db_ref, db),
        ])
    ]
    for copy in loads[:4]:
        copy.start()

    def slot(kind, h):
        return table.at[kind, h]

    def own_source(kind):
        return (asc_ref if kind == ASC else desc_ref).at[0, 3]

    def send(kind, h, i, src):
        return pltpu.make_async_remote_copy(
            src_ref=src, dst_ref=slot(kind, h),
            send_sem=gen_send.at[kind, h, i], recv_sem=gen_recv.at[kind, h],
            device_id=partner[i], device_id_type=MESH,
        )

    def wait_slot(kind, h):
        pltpu.make_async_copy(slot(kind, h), slot(kind, h), gen_recv.at[kind, h]).wait()

    def owner_local(kind, h):
        if kind == COUP:
            for n, k in enumerate((0, 3)):
                pltpu.make_async_copy(
                    coup_ref.at[0, 1, k], table.at[COUP, h, n], gen_recv.at[COUP, h]
                ).start()
        else:
            pltpu.make_async_copy(own_source(kind), slot(kind, h), gen_recv.at[kind, h]).start()

    pl.semaphore_wait(barrier, levels)

    for h in range(1, levels + 1):
        @pl.when(count[h] == 0)
        def _(h=h):
            for kind in (ASC, DESC, COUP):
                if h > last[kind]:
                    continue
                if kind == COUP:
                    send(kind, h, h - 1, coup_ref.at[0, 1, 1:3]).start()
                else:
                    for i in reversed(range(h)):
                        send(kind, h, i, own_source(kind)).start()
                owner_local(kind, h)

    def forwards(k, kinds):
        for kind in kinds:
            for h in range(2, last[kind] + 1):
                if k > h - 1 or (k == 0 and kind != COUP):
                    continue

                @pl.when((count[h] == k) & (low_sum[h, 0] == 0))
                def _(kind=kind, h=h):
                    wait_slot(kind, h)
                    for i in reversed(range(h - 1)):
                        @pl.when(low_sum[h, i] == 0)
                        def _(i=i):
                            send(kind, h, i, slot(kind, h)).start()

    def ready(kind, h):
        if h == 1:
            wait_slot(kind, h)
            return
        waited = low_sum[h, 0] == 0
        if kind != COUP:
            waited = waited & (count[h] > 0)

        @pl.when(jnp.logical_not(waited))
        def _():
            wait_slot(kind, h)

    def up_copy(which, h):
        src, dst = ((f_out, f_in), (t_out, t_in))[which]
        return pltpu.make_async_remote_copy(
            src_ref=src.at[h], dst_ref=dst.at[h],
            send_sem=up_send.at[which, h], recv_sem=up_recv.at[which, h],
            device_id=partner[h], device_id_type=MESH,
        )

    def near(h):
        ready(COUP, h)
        up_copy(0, h - 1).wait()
        pair = slot(COUP, h)
        return across(pair[0], f_in[h - 1], pair[1])

    for copy in loads[4:]:
        copy.start()
    loads[0].wait()
    leaf = [mm(inner[u, 0], inner[u, 1], 0, 0) for u in range(2)]
    loads[1].wait()
    node = lift(own_asc.at[0], leaf[0]) + lift(own_asc.at[1], leaf[1])
    done = 0
    for h in range(levels):
        f_out[h] = node.astype(BF16)
        up_copy(0, h).start()
        if h < levels - 1:
            if h == 0:
                pair = own_asc.at[2]
            else:
                ready(ASC, h)
                pair = slot(ASC, h)
            term = lift(pair, node)
            t_out[h] = term.astype(BF16)
            up_copy(1, h).start()
        if h == 0:
            loads[2].wait()
            near_leaf[0] = across(own_coup[0], leaf[1], own_coup[3])
            near_leaf[1] = across(own_coup[1], leaf[0], own_coup[2])
        if h == min(1, levels - 1):
            loads[5].wait()
            loads[6].wait()
            for u in range(2):
                dense[u] = mm(da[u], db[u])
        forwards(h + 1, (ASC,))
        forwards(h, (DESC, COUP))
        while done < h - 1:
            done += 1
            near_up[done - 1] = near(done)
        if h < levels - 1:
            up_copy(1, h).wait()
            node = term + t_in[h].astype(F32)

    loads[3].wait()
    loads[4].wait()
    while done < levels - 1:
        done += 1
        near_up[done - 1] = near(done)
    for h in range(1, levels - 1):
        ready(DESC, h)
    coupling = near(levels)
    for h in range(levels - 2, -1, -1):
        pair = slot(DESC, h) if h else own_desc.at[2]
        coupling = near_up[h] + lower(pair, coupling)
    stores = []
    for u in range(2):
        value = (near_leaf[u] + lower(own_desc.at[u], coupling)).astype(BF16)
        spread = mm(outer[u, 0], value).astype(BF16)
        out[u] = (dense[u] + mm(spread, outer[u, 1], 1, 1)).astype(BF16)
        store = pltpu.make_async_copy(out.at[u], o_ref.at[u], out_sem.at[u])
        store.start()
        stores.append(store)

    for h in range(1, levels + 1):
        for kind in (ASC, DESC, COUP):
            if h > last[kind]:
                continue
            for i in range(h):
                if i == h - 1:
                    sent = count[h] == 0
                else:
                    sent = low_sum[h, i] == 0

                @pl.when(sent)
                def _(kind=kind, h=h, i=i):
                    send(kind, h, i, slot(kind, h)).wait_send()
    for store in stores:
        store.wait()


def shards(levels, columns, dense_a, dense_b, inner, outer, ascent, descent, couplings):
    r = ascent.shape[-1]
    anywhere = pl.BlockSpec(memory_space=pl.ANY)
    vmem = pltpu.VMEM
    dma = pltpu.SemaphoreType.DMA
    return pl.pallas_call(
        functools.partial(tree_kernel, levels, columns),
        out_shape=jax.ShapeDtypeStruct(dense_a.shape, BF16),
        in_specs=[anywhere] * 7,
        out_specs=anywhere,
        scratch_shapes=[
            vmem(dense_a.shape, BF16),
            vmem(dense_b.shape, BF16),
            vmem(inner.shape, BF16),
            vmem(outer.shape, BF16),
            vmem(ascent.shape[1:], BF16),
            vmem(descent.shape[1:], BF16),
            vmem(couplings.shape[2:], BF16),
            vmem(dense_a.shape, BF16),
            vmem(dense_a.shape, F32),
            vmem((3, levels + 1, 2, r, r), BF16),
            vmem((levels, r, r), BF16),
            vmem((levels, r, r), BF16),
            vmem((levels, r, r), BF16),
            vmem((levels, r, r), BF16),
            vmem((2, r, r), F32),
            vmem((levels, r, r), F32),
            dma((7,)),
            dma((2,)),
            dma((3, levels + 1, levels)),
            dma((3, levels + 1)),
            dma((2, levels)),
            dma((2, levels)),
        ],
        compiler_params=pltpu.CompilerParams(collective_id=0, has_side_effects=True),
    )(dense_a, dense_b, inner, outer, ascent, descent, couplings)


def solution(mesh):
    rows, columns = mesh.shape["row"], mesh.shape["col"]
    levels = (rows * columns).bit_length() - 1
    both = ("row", "col")
    placed = (
        P(both, None, None),
        P(both, None, None),
        P(both, None, None, None),
        P(both, None, None, None),
        P(both, None, None, None, None),
        P(both, None, None, None, None),
        P(both, None, None, None, None),
    )
    return jax.shard_map(
        functools.partial(shards, levels, columns),
        mesh=mesh, in_specs=placed, out_specs=P(both, None, None), check_vma=False,
    )
```

```python
import functools

import jax
import jax.numpy as jnp
from jax import lax
from jax.experimental import pallas as pl
from jax.experimental.pallas import tpu as pltpu
from jax.sharding import PartitionSpec as P

MESH = pl.DeviceIdType.MESH
BF16 = jnp.bfloat16
F32 = jnp.float32
ASC, DESC, COUP = 0, 1, 2


def mm(a, b, ca=1, cb=0):
    return lax.dot_general(
        a.astype(BF16), b.astype(BF16), (((ca,), (cb,)), ((), ())), preferred_element_type=F32
    )


def halves(value):
    high = value.astype(BF16)
    return high, (value - high.astype(F32)).astype(BF16)


def times(value, factor, cb=0):
    if value.dtype == BF16:
        return mm(value, factor, 1, cb)
    rows = value.shape[0]
    both = mm(jnp.concatenate(halves(value), 0), factor, 1, cb)
    return both[:rows] + both[rows:]


def into(factor, value, ca=1):
    if value.dtype == BF16:
        return mm(factor, value, ca, 0)
    columns = value.shape[1]
    both = mm(factor, jnp.concatenate(halves(value), 1), ca, 0)
    return both[:, :columns] + both[:, columns:]


def lift(pair, value):
    return into(pair[0], times(value, pair[1]), 0)


def lower(pair, value):
    return times(into(pair[0], value), pair[1], 1)


def across(first, value, second):
    return times(into(first, value), second)


def tree_kernel(
    levels, columns,
    da_ref, db_ref, inner_ref, outer_ref, asc_ref, desc_ref, coup_ref, o_ref,
    da, db, inner, outer, own_asc, own_desc, own_coup, out, dense,
    table, f_out, t_out, f_in, t_in, near_leaf, near_up,
    comp, far_in,
    load_sem, out_sem, gen_send, gen_recv, up_send, up_recv, far_send, far_recv,
):
    pos = lax.axis_index("row") * columns + lax.axis_index("col")
    bit = [pos // 2**i % 2 for i in range(levels)]
    partner = []
    for i in range(levels):
        other = pos + 2**i * (1 - 2 * bit[i])
        partner.append((other // columns, other % columns))

    top = levels - 1
    far = pos + 2**top * (1 - 2 * bit[top])
    cross = far + 2 ** (top - 1) * (1 - 2 * bit[top - 1])
    opposite = (partner[top], (cross // columns, cross % columns))

    low_sum = {}
    for h in range(1, levels + 1):
        total = 0
        for i in range(h):
            total = total + (bit[i] if i == h - 1 else 1 - bit[i])
            low_sum[h, i] = total
    count = {h: low_sum[h, h - 1] for h in range(1, levels + 1)}
    last = {ASC: levels - 2, DESC: levels - 2, COUP: levels}

    barrier = pltpu.get_barrier_semaphore()
    for other in [*partner, opposite[1]]:
        pl.semaphore_signal(barrier, inc=1, device_id=other, device_id_type=MESH)

    loads = [
        pltpu.make_async_copy(src, dst, load_sem.at[n])
        for n, (src, dst) in enumerate([
            (inner_ref, inner),
            (asc_ref.at[0], own_asc),
            (coup_ref.at[0, 0], own_coup),
            (desc_ref.at[0], own_desc),
            (outer_ref, outer),
            (da_ref, da),
            (db_ref, db),
        ])
    ]
    for copy in loads[:4]:
        copy.start()

    def slot(kind, h):
        return table.at[kind, h]

    def own_source(kind):
        return (asc_ref if kind == ASC else desc_ref).at[0, 3]

    def send(kind, h, i, src):
        return pltpu.make_async_remote_copy(
            src_ref=src, dst_ref=slot(kind, h),
            send_sem=gen_send.at[kind, h, i], recv_sem=gen_recv.at[kind, h],
            device_id=partner[i], device_id_type=MESH,
        )

    def wait_slot(kind, h):
        pltpu.make_async_copy(slot(kind, h), slot(kind, h), gen_recv.at[kind, h]).wait()

    def owner_local(kind, h):
        if kind == COUP:
            for n, k in enumerate((0, 3)):
                pltpu.make_async_copy(
                    coup_ref.at[0, 1, k], table.at[COUP, h, n], gen_recv.at[COUP, h]
                ).start()
        else:
            pltpu.make_async_copy(own_source(kind), slot(kind, h), gen_recv.at[kind, h]).start()

    def forwards(k, kinds):
        for kind in kinds:
            for h in range(2, last[kind] + 1):
                if k > h - 1 or (k == 0 and kind != COUP):
                    continue

                @pl.when((count[h] == k) & (low_sum[h, 0] == 0))
                def _(kind=kind, h=h):
                    wait_slot(kind, h)
                    for i in reversed(range(h - 1)):
                        @pl.when(low_sum[h, i] == 0)
                        def _(i=i):
                            send(kind, h, i, slot(kind, h)).start()

    def ready(kind, h):
        if h == 1:
            wait_slot(kind, h)
            return
        waited = low_sum[h, 0] == 0
        if kind != COUP:
            waited = waited & (count[h] > 0)

        @pl.when(jnp.logical_not(waited))
        def _():
            wait_slot(kind, h)

    def up_copy(which, h):
        src, dst = ((f_out, f_in), (t_out, t_in))[which]
        return pltpu.make_async_remote_copy(
            src_ref=src.at[h], dst_ref=dst.at[h],
            send_sem=up_send.at[which, h], recv_sem=up_recv.at[which, h],
            device_id=partner[h], device_id_type=MESH,
        )

    def near(h):
        ready(COUP, h)
        up_copy(0, h - 1).wait()
        pair = slot(COUP, h)
        return across(pair[0], f_in[h - 1], pair[1])

    def far_copy(n):
        return pltpu.make_async_remote_copy(
            src_ref=t_out.at[top - 1], dst_ref=far_in.at[n],
            send_sem=far_send.at[n], recv_sem=far_recv.at[n],
            device_id=opposite[n], device_id_type=MESH,
        )

    def compose(n, left, right, h):
        ready(COUP, h)
        pair = slot(COUP, h)
        for u in range(2):
            comp[n, 0, u] = times(into(own_desc[u, 0], left), pair[0]).astype(BF16)
            high, low = halves(into(own_desc[u, 1], right))
            comp[n, 1, u] = (mm(pair[1], high, 1, 1) + mm(pair[1], low, 1, 1)).astype(BF16)

    pl.semaphore_wait(barrier, levels + 1)

    for h in range(1, levels + 1):
        @pl.when(count[h] == 0)
        def _(h=h):
            for kind in (ASC, DESC, COUP):
                if h > last[kind]:
                    continue
                if kind == COUP:
                    send(kind, h, h - 1, coup_ref.at[0, 1, 1:3]).start()
                else:
                    for i in reversed(range(h)):
                        send(kind, h, i, own_source(kind)).start()
                owner_local(kind, h)

    loads[0].wait()
    for copy in loads[4:]:
        copy.start()
    leaf = [mm(inner[u, 0], inner[u, 1], 0, 0) for u in range(2)]
    loads[1].wait()
    node = lift(own_asc.at[0], leaf[0]) + lift(own_asc.at[1], leaf[1])
    term = lift(own_asc.at[2], node)
    f_out[0] = node.astype(BF16)
    t_out[0] = term.astype(BF16)

    done = 0
    for h in range(top):
        if h > 0:
            ready(ASC, h)
            term = lift(slot(ASC, h), node)
            t_out[h] = term.astype(BF16)
        if h < top - 1:
            up_copy(1, h).start()
        else:
            far_copy(1).start()
            far_copy(0).start()
        if h > 0:
            f_out[h] = node.astype(BF16)
        up_copy(0, h).start()
        if h == 0:
            loads[2].wait()
            near_leaf[0] = across(own_coup[0], leaf[1], own_coup[3])
            near_leaf[1] = across(own_coup[1], leaf[0], own_coup[2])
        if h == min(1, top - 1):
            loads[5].wait()
            loads[6].wait()
            for u in range(2):
                dense[u] = mm(da[u], db[u])
        forwards(h + 1, (ASC,))
        forwards(h, (DESC, COUP))
        while done < h - 1:
            done += 1
            near_up[done - 1] = near(done)
        if h < top - 1:
            up_copy(1, h).wait()
            node = term + t_in[h].astype(F32)

    for k in range(top, levels):
        forwards(k, (DESC, COUP))
    loads[3].wait()
    loads[4].wait()
    while done < top - 1:
        done += 1
        near_up[done - 1] = near(done)
    for h in range(1, top):
        ready(DESC, h)
    coupling = near_up[top - 2]
    for h in range(top - 3, -1, -1):
        coupling = near_up[h] + lower(slot(DESC, h) if h else own_desc.at[2], coupling)
    for u in range(2):
        near_leaf[u] += lower(own_desc.at[u], coupling)

    left, right = own_desc[2, 0], own_desc[2, 1]
    for h in range(1, top - 1):
        left, right = times(left, table[DESC, h, 0]), times(right, table[DESC, h, 1])
    compose(0, left, right, top)
    left, right = times(left, table[DESC, top - 1, 0]), times(right, table[DESC, top - 1, 1])
    compose(1, left, right, levels)

    up_copy(0, top - 1).wait()
    for u in range(2):
        near_leaf[u] += mm(mm(comp[0, 0, u], f_in[top - 1]), comp[0, 1, u])
    for n in (0, 1):
        far_copy(n).wait()
    last_inner = (far_in[0].astype(F32) + far_in[1].astype(F32)).astype(BF16)
    stores = []
    for u in range(2):
        value = (near_leaf[u] + mm(mm(comp[1, 0, u], last_inner), comp[1, 1, u])).astype(BF16)
        spread = mm(outer[u, 0], value).astype(BF16)
        out[u] = (dense[u] + mm(spread, outer[u, 1], 1, 1)).astype(BF16)
        store = pltpu.make_async_copy(out.at[u], o_ref.at[u], out_sem.at[u])
        store.start()
        stores.append(store)

    for h in range(1, levels + 1):
        for kind in (ASC, DESC, COUP):
            if h > last[kind]:
                continue
            for i in range(h):
                if i == h - 1:
                    sent = count[h] == 0
                else:
                    sent = low_sum[h, i] == 0

                @pl.when(sent)
                def _(kind=kind, h=h, i=i):
                    send(kind, h, i, slot(kind, h)).wait_send()
    for store in stores:
        store.wait()


def shards(levels, columns, dense_a, dense_b, inner, outer, ascent, descent, couplings):
    r = ascent.shape[-1]
    arrays = (dense_a, dense_b, inner, outer, ascent, descent, couplings)
    anywhere = pl.BlockSpec(memory_space=pl.ANY)
    vmem = pltpu.VMEM
    dma = pltpu.SemaphoreType.DMA
    return pl.pallas_call(
        functools.partial(tree_kernel, levels, columns),
        out_shape=jax.ShapeDtypeStruct(dense_a.shape, BF16),
        in_specs=[pl.BlockSpec(memory_space=pltpu.HBM)] * 7,
        out_specs=anywhere,
        scratch_shapes=[
            vmem(dense_a.shape, BF16),
            vmem(dense_b.shape, BF16),
            vmem(inner.shape, BF16),
            vmem(outer.shape, BF16),
            vmem(ascent.shape[1:], BF16),
            vmem(descent.shape[1:], BF16),
            vmem(couplings.shape[2:], BF16),
            vmem(dense_a.shape, BF16),
            vmem(dense_a.shape, F32),
            vmem((3, levels + 1, 2, r, r), BF16),
            vmem((levels, r, r), BF16),
            vmem((levels, r, r), BF16),
            vmem((levels, r, r), BF16),
            vmem((levels, r, r), BF16),
            vmem((2, r, r), F32),
            vmem((levels, r, r), F32),
            vmem((2, 2, 2, r, r), BF16),
            vmem((2, r, r), BF16),
            dma((7,)),
            dma((2,)),
            dma((3, levels + 1, levels)),
            dma((3, levels + 1)),
            dma((2, levels)),
            dma((2, levels)),
            dma((2,)),
            dma((2,)),
        ],
        compiler_params=pltpu.CompilerParams(collective_id=0, has_side_effects=True, vmem_limit_bytes=24 * 2**20),
    )(*(pltpu.with_memory_space_constraint(x, pltpu.HBM) for x in arrays))


def solution(mesh):
    rows, columns = mesh.shape["row"], mesh.shape["col"]
    levels = (rows * columns).bit_length() - 1
    both = ("row", "col")
    placed = (
        P(both, None, None),
        P(both, None, None),
        P(both, None, None, None),
        P(both, None, None, None),
        P(both, None, None, None, None),
        P(both, None, None, None, None),
        P(both, None, None, None, None),
    )
    return jax.shard_map(
        functools.partial(shards, levels, columns),
        mesh=mesh, in_specs=placed, out_specs=P(both, None, None), check_vma=False,
    )
```

```python
import functools

import jax
import jax.numpy as jnp
from jax import lax
from jax.experimental import pallas as pl
from jax.experimental.pallas import tpu as pltpu
from jax.sharding import PartitionSpec as P

MESH = pl.DeviceIdType.MESH
BF16 = jnp.bfloat16
F32 = jnp.float32
ASC, DESC, COUP = 0, 1, 2


def mm(a, b, ca=1, cb=0):
    return lax.dot_general(
        a.astype(BF16), b.astype(BF16), (((ca,), (cb,)), ((), ())), preferred_element_type=F32
    )


def halves(value):
    high = value.astype(BF16)
    return high, (value - high.astype(F32)).astype(BF16)


def times(value, factor, cb=0):
    if value.dtype == BF16:
        return mm(value, factor, 1, cb)
    rows = value.shape[0]
    both = mm(jnp.concatenate(halves(value), 0), factor, 1, cb)
    return both[:rows] + both[rows:]


def into(factor, value, ca=1):
    if value.dtype == BF16:
        return mm(factor, value, ca, 0)
    columns = value.shape[1]
    both = mm(factor, jnp.concatenate(halves(value), 1), ca, 0)
    return both[:, :columns] + both[:, columns:]


def lift(pair, value):
    return into(pair[0], times(value, pair[1]), 0)


def lower(pair, value):
    return times(into(pair[0], value), pair[1], 1)


def across(first, value, second):
    return times(into(first, value), second)


def tree_kernel(
    levels, columns,
    da_ref, db_ref, inner_ref, outer_ref, asc_ref, desc_ref, coup_ref, o_ref,
    da, db, inner, outer, own_asc, own_desc, own_coup, dense,
    table, f_out, t_out, f_in, t_in, near_leaf, near_up,
    comp, far_in,
    load_sem, gen_send, gen_recv, up_send, up_recv, far_send, far_recv,
):
    pos = lax.axis_index("row") * columns + lax.axis_index("col")
    bit = [pos // 2**i % 2 for i in range(levels)]
    partner = []
    for i in range(levels):
        other = pos + 2**i * (1 - 2 * bit[i])
        partner.append((other // columns, other % columns))

    top = levels - 1
    far = pos + 2**top * (1 - 2 * bit[top])
    cross = far + 2 ** (top - 1) * (1 - 2 * bit[top - 1])
    opposite = (partner[top], (cross // columns, cross % columns))

    low_sum = {}
    for h in range(1, levels + 1):
        total = 0
        for i in range(h):
            total = total + (bit[i] if i == h - 1 else 1 - bit[i])
            low_sum[h, i] = total
    count = {h: low_sum[h, h - 1] for h in range(1, levels + 1)}
    last = {ASC: levels - 2, DESC: levels - 2, COUP: levels}

    barrier = pltpu.get_barrier_semaphore()
    for other in [*partner, opposite[1]]:
        pl.semaphore_signal(barrier, inc=1, device_id=other, device_id_type=MESH)

    loads = [
        pltpu.make_async_copy(src, dst, load_sem.at[n])
        for n, (src, dst) in enumerate([
            (inner_ref, inner),
            (asc_ref.at[0], own_asc),
            (coup_ref.at[0, 0], own_coup),
            (desc_ref.at[0], own_desc),
            (outer_ref, outer),
            (da_ref, da),
            (db_ref, db),
        ])
    ]
    for copy in loads[:4]:
        copy.start()

    def slot(kind, h):
        return table.at[kind, h]

    def own_source(kind):
        return (asc_ref if kind == ASC else desc_ref).at[0, 3]

    def send(kind, h, i, src):
        return pltpu.make_async_remote_copy(
            src_ref=src, dst_ref=slot(kind, h),
            send_sem=gen_send.at[kind, h, i], recv_sem=gen_recv.at[kind, h],
            device_id=partner[i], device_id_type=MESH,
        )

    def wait_slot(kind, h):
        pltpu.make_async_copy(slot(kind, h), slot(kind, h), gen_recv.at[kind, h]).wait()

    def owner_local(kind, h):
        if kind == COUP:
            for n, k in enumerate((0, 3)):
                pltpu.make_async_copy(
                    coup_ref.at[0, 1, k], table.at[COUP, h, n], gen_recv.at[COUP, h]
                ).start()
        else:
            pltpu.make_async_copy(own_source(kind), slot(kind, h), gen_recv.at[kind, h]).start()

    def forwards(k, kinds):
        for kind in kinds:
            for h in range(2, last[kind] + 1):
                if k > h - 1 or (k == 0 and kind != COUP):
                    continue

                @pl.when((count[h] == k) & (low_sum[h, 0] == 0))
                def _(kind=kind, h=h):
                    wait_slot(kind, h)
                    for i in reversed(range(h - 1)):
                        @pl.when(low_sum[h, i] == 0)
                        def _(i=i):
                            send(kind, h, i, slot(kind, h)).start()

    def ready(kind, h):
        if h == 1:
            wait_slot(kind, h)
            return
        waited = low_sum[h, 0] == 0
        if kind != COUP:
            waited = waited & (count[h] > 0)

        @pl.when(jnp.logical_not(waited))
        def _():
            wait_slot(kind, h)

    def up_copy(which, h):
        src, dst = ((f_out, f_in), (t_out, t_in))[which]
        return pltpu.make_async_remote_copy(
            src_ref=src.at[h], dst_ref=dst.at[h],
            send_sem=up_send.at[which, h], recv_sem=up_recv.at[which, h],
            device_id=partner[h], device_id_type=MESH,
        )

    def near(h):
        ready(COUP, h)
        up_copy(0, h - 1).wait()
        pair = slot(COUP, h)
        return across(pair[0], f_in[h - 1], pair[1])

    def far_copy(n):
        return pltpu.make_async_remote_copy(
            src_ref=t_out.at[top - 1], dst_ref=far_in.at[n],
            send_sem=far_send.at[n], recv_sem=far_recv.at[n],
            device_id=opposite[n], device_id_type=MESH,
        )

    def compose(n, left, right, h):
        ready(COUP, h)
        pair = slot(COUP, h)
        for u in range(2):
            comp[n, 0, u] = times(into(own_desc[u, 0], left), pair[0]).astype(BF16)
            high, low = halves(into(own_desc[u, 1], right))
            comp[n, 1, u] = (mm(pair[1], high, 1, 1) + mm(pair[1], low, 1, 1)).astype(BF16)

    pl.semaphore_wait(barrier, levels + 1)

    for h in range(1, levels + 1):
        @pl.when(count[h] == 0)
        def _(h=h):
            for kind in (ASC, DESC, COUP):
                if h > last[kind]:
                    continue
                if kind == COUP:
                    send(kind, h, h - 1, coup_ref.at[0, 1, 1:3]).start()
                else:
                    for i in reversed(range(h)):
                        send(kind, h, i, own_source(kind)).start()
                owner_local(kind, h)

    loads[0].wait()
    for copy in loads[4:]:
        copy.start()
    leaf = [mm(inner[u, 0], inner[u, 1], 0, 0) for u in range(2)]
    loads[1].wait()
    node = lift(own_asc.at[0], leaf[0]) + lift(own_asc.at[1], leaf[1])
    term = lift(own_asc.at[2], node)
    f_out[0] = node.astype(BF16)
    t_out[0] = term.astype(BF16)

    done = 0
    for h in range(top):
        if h > 0:
            ready(ASC, h)
            term = lift(slot(ASC, h), node)
            t_out[h] = term.astype(BF16)
        if h < top - 1:
            up_copy(1, h).start()
        else:
            far_copy(1).start()
            far_copy(0).start()
        if h > 0:
            f_out[h] = node.astype(BF16)
        up_copy(0, h).start()
        if h == 0:
            loads[2].wait()
            near_leaf[0] = across(own_coup[0], leaf[1], own_coup[3])
            near_leaf[1] = across(own_coup[1], leaf[0], own_coup[2])
        if h == 1:
            loads[5].wait()
            loads[6].wait()
        if h in (1, 2):
            dense[h - 1] = mm(da[h - 1], db[h - 1])
        forwards(h + 1, (ASC,))
        forwards(h - 1, (DESC, COUP))
        while done < h - 1:
            done += 1
            near_up[done - 1] = near(done)
        if h < top - 1:
            up_copy(1, h).wait()
            node = term + t_in[h].astype(F32)

    for k in range(top - 1, levels):
        forwards(k, (DESC, COUP))
    loads[3].wait()
    loads[4].wait()
    while done < top - 1:
        done += 1
        near_up[done - 1] = near(done)
    for h in range(1, top):
        ready(DESC, h)
    coupling = near_up[top - 2]
    for h in range(top - 3, -1, -1):
        coupling = near_up[h] + lower(slot(DESC, h) if h else own_desc.at[2], coupling)
    for u in range(2):
        near_leaf[u] += lower(own_desc.at[u], coupling)

    left, right = own_desc[2, 0], own_desc[2, 1]
    for h in range(1, top - 1):
        left, right = times(left, table[DESC, h, 0]), times(right, table[DESC, h, 1])
    compose(0, left, right, top)
    left, right = times(left, table[DESC, top - 1, 0]), times(right, table[DESC, top - 1, 1])
    compose(1, left, right, levels)

    up_copy(0, top - 1).wait()
    for u in range(2):
        near_leaf[u] += mm(mm(comp[0, 0, u], f_in[top - 1]), comp[0, 1, u])
    for n in (0, 1):
        far_copy(n).wait()
    last_inner = (far_in[0].astype(F32) + far_in[1].astype(F32)).astype(BF16)
    for u in range(2):
        value = (near_leaf[u] + mm(mm(comp[1, 0, u], last_inner), comp[1, 1, u])).astype(BF16)
        spread = mm(outer[u, 0], value).astype(BF16)
        o_ref[u] = (dense[u] + mm(spread, outer[u, 1], 1, 1)).astype(BF16)

    for h in range(1, levels + 1):
        for kind in (ASC, DESC, COUP):
            if h > last[kind]:
                continue
            for i in range(h):
                if i == h - 1:
                    sent = count[h] == 0
                else:
                    sent = low_sum[h, i] == 0

                @pl.when(sent)
                def _(kind=kind, h=h, i=i):
                    send(kind, h, i, slot(kind, h)).wait_send()


def shards(levels, columns, dense_a, dense_b, inner, outer, ascent, descent, couplings):
    r = ascent.shape[-1]
    arrays = (dense_a, dense_b, inner, outer, ascent, descent, couplings)
    vmem = pltpu.VMEM
    dma = pltpu.SemaphoreType.DMA
    return pl.pallas_call(
        functools.partial(tree_kernel, levels, columns),
        out_shape=jax.ShapeDtypeStruct(dense_a.shape, BF16),
        in_specs=[pl.BlockSpec(memory_space=pltpu.HBM)] * 7,
        out_specs=pl.BlockSpec(memory_space=pltpu.VMEM),
        scratch_shapes=[
            vmem(dense_a.shape, BF16),
            vmem(dense_b.shape, BF16),
            vmem(inner.shape, BF16),
            vmem(outer.shape, BF16),
            vmem(ascent.shape[1:], BF16),
            vmem(descent.shape[1:], BF16),
            vmem(couplings.shape[2:], BF16),
            vmem(dense_a.shape, F32),
            vmem((3, levels + 1, 2, r, r), BF16),
            vmem((levels, r, r), BF16),
            vmem((levels, r, r), BF16),
            vmem((levels, r, r), BF16),
            vmem((levels, r, r), BF16),
            vmem((2, r, r), F32),
            vmem((levels, r, r), F32),
            vmem((2, 2, 2, r, r), BF16),
            vmem((2, r, r), BF16),
            dma((7,)),
            dma((3, levels + 1, levels)),
            dma((3, levels + 1)),
            dma((2, levels)),
            dma((2, levels)),
            dma((2,)),
            dma((2,)),
        ],
        compiler_params=pltpu.CompilerParams(collective_id=0, has_side_effects=True, vmem_limit_bytes=24 * 2**20),
    )(*(pltpu.with_memory_space_constraint(x, pltpu.HBM) for x in arrays))


def solution(mesh):
    rows, columns = mesh.shape["row"], mesh.shape["col"]
    levels = (rows * columns).bit_length() - 1
    both = ("row", "col")
    placed = (
        P(both, None, None),
        P(both, None, None),
        P(both, None, None, None),
        P(both, None, None, None),
        P(both, None, None, None, None),
        P(both, None, None, None, None),
        P(both, None, None, None, None),
    )
    return jax.shard_map(
        functools.partial(shards, levels, columns),
        mesh=mesh, in_specs=placed, out_specs=P(both, None, None), check_vma=False,
    )
```
